32 devices in a mesh: seq: 8 (over z, y), head: 4 (over x, core).
Axes of the slice: x: 2, y: 2, z: 4, core: 2. Of those that a mesh axis runs over, the one named last changes fastest.
Arguments:
- queries: bfloat16 [2048, 4096], P('seq', 'head'), may hold values from -5 to 5
- keys: bfloat16 [2048, 4096], P('seq', 'head'), may hold values from -5 to 5
- values: bfloat16 [2048, 4096], P('seq', 'head'), may hold values from -6 to 6
- beta: float32 [32], P('head'), may hold values from -2 to 2
- w_out: bfloat16 [4096, 4096], P('head'), may hold values from -0.09375 to 0.09375
Outputs:
- mixed: bfloat16 [2048, 4096], P('seq', 'head')
The draws below stay inside these ranges and needn't reach their ends.
All inputs are finite; a program needn't handle non-finite values.
Results may differ from the reference program's by a relative error of at most 0.0069.
Values may be sent and summed in bfloat16 or wider, within the bound.
A program may use at most 192 MiB of HBM per device.

```python
import jax
import jax.numpy as jnp
from jax import lax

D = 4096
HEADS = 32
HD = 128
SEG = 2048
TOKENS = 2048


def draw_queries(key, part):
    own_key = jax.random.fold_in(key, 11)
    extent = (TOKENS, HEADS * HD)
    base = jnp.clip(0.7 * jax.random.normal(own_key, extent, jnp.float32), -5.0, 5.0)
    return base.astype(jnp.bfloat16)


def draw_keys(key, part):
    own_key = jax.random.fold_in(key, 12)
    extent = (TOKENS, HEADS * HD)
    position = jnp.arange(TOKENS)
    rising = (3.0 * position.astype(jnp.float32) / TOKENS)[:, None]
    base = jnp.clip(jax.random.normal(own_key, extent, jnp.float32) + rising, -5.0, 5.0)
    return base.astype(jnp.bfloat16)


def draw_values(key, part):
    own_key = jax.random.fold_in(key, 13)
    extent = (TOKENS, HEADS * HD)
    segments = TOKENS // SEG
    offsets = jax.random.normal(jax.random.fold_in(key, 14), (segments, HEADS * HD), jnp.float32)
    noise = jax.random.normal(own_key, extent, jnp.float32)
    spread = jnp.repeat(offsets, SEG, axis=0)
    return jnp.clip(0.8 * noise + 0.8 * spread, -6.0, 6.0).astype(jnp.bfloat16)


def steps_of(key, shape, split, low, largest):
    loudness = 1.0
    for dim, shards_of in split:
        draws = jax.random.uniform(jax.random.fold_in(jax.random.fold_in(key, 6), dim), (shards_of,), jnp.float32, low / len(split), largest / len(split))
        loudness = loudness * jnp.repeat(jnp.exp(draws), shape[dim] // shards_of).reshape((-1,) + (1,) * (len(shape) - 1 - dim))
    return loudness


def gaussian(key, shape, scale, bound, pieces=(), held_as=jnp.bfloat16):
    values = scale * jax.random.normal(key, shape, jnp.float32)
    if pieces:
        values = values * steps_of(key, shape, pieces, -0.22, 0.18)
    return jnp.clip(values, -bound, bound).astype(held_as)


def setup_inputs(seed: int = 0) -> dict:
    streams_of = jax.random.split(jax.random.key(seed), 6)
    queries = draw_queries(jax.random.fold_in(streams_of[5], 71), 0)
    keys = draw_keys(jax.random.fold_in(streams_of[5], 71), 0)
    values = draw_values(jax.random.fold_in(streams_of[5], 71), 0)
    beta = jnp.clip(jax.random.uniform(streams_of[3], (HEADS,), jnp.float32, -2.0, 2.0) * steps_of(streams_of[3], (HEADS,), ((0, 4),), -0.4, 0.0), -2.0, 2.0)
    w_out = gaussian(streams_of[4], (HEADS * HD, D), (HEADS * HD) ** -0.5, 0.09375, ((0, 4),))
    return dict(queries=queries, keys=keys, values=values, beta=beta, w_out=w_out)


def elu_plus(inputs):
    return jnp.where(inputs > 0, inputs + 1.0, jnp.exp(jnp.minimum(inputs, 0.0)))


def window_head(packed):
    query_head, key_head, value_head, first_flag = packed
    scores = jnp.dot(query_head, key_head.T, preferred_element_type=jnp.float32) * (HD ** -0.5)
    query_pos = jnp.arange(SEG)[:, None] + SEG
    key_pos = jnp.arange(2 * SEG)[None, :]
    visible = (key_pos <= query_pos) & (key_pos > query_pos - SEG) & ((key_pos >= SEG) | (first_flag < 1))
    scores = jnp.where(visible, scores, -jnp.inf)
    highest = jnp.max(scores, axis=-1, keepdims=True)
    weights = jnp.exp(scores - highest)
    total = jnp.sum(weights, axis=-1, keepdims=True)
    rounded = weights.astype(jnp.bfloat16)
    summed = jnp.dot(rounded, value_head, preferred_element_type=jnp.float32)
    return summed / total


def segment_attention(packed):
    query_seg, key_seg, value_seg, key_prev, value_prev, first_flag = packed
    key_both = jnp.concatenate([key_prev, key_seg], axis=0)
    value_both = jnp.concatenate([value_prev, value_seg], axis=0)
    flags = jnp.full((HEADS,), first_flag, jnp.int32)
    result = lax.map(window_head, (jnp.transpose(query_seg, (1, 0, 2)), jnp.transpose(key_both, (1, 0, 2)), jnp.transpose(value_both, (1, 0, 2)), flags))
    return jnp.transpose(result, (1, 0, 2))


def segment_terms(packed):
    key_seg, value_seg = packed
    soft_keys = elu_plus(key_seg.astype(jnp.float32)).astype(jnp.bfloat16)
    outer = jnp.einsum("thd,the->hde", soft_keys.astype(jnp.float32), value_seg.astype(jnp.float32))
    totals = jnp.sum(soft_keys.astype(jnp.float32), axis=0)
    return outer, totals


def reference(queries, keys, values, beta, w_out):
    segments = TOKENS // SEG
    shaped = (segments, SEG, HEADS, HD)
    query_all = queries.reshape(shaped)
    key_all = keys.reshape(shaped)
    value_all = values.reshape(shaped)
    terms, norms = lax.map(segment_terms, (key_all, value_all))
    memory = jnp.concatenate([jnp.zeros((1, HEADS, HD, HD), jnp.float32), jnp.cumsum(terms, axis=0)[:-1]], axis=0)
    norm_prev = jnp.concatenate([jnp.zeros((1, HEADS, HD), jnp.float32), jnp.cumsum(norms, axis=0)[:-1]], axis=0)
    soft_queries = lax.optimization_barrier(elu_plus(query_all.astype(jnp.float32)).astype(jnp.bfloat16)).astype(jnp.float32)
    numer = jnp.einsum("sthd,shde->sthe", soft_queries, memory, precision=lax.Precision.HIGHEST)
    denom = 1.0 + jnp.einsum("sthd,shd->sth", soft_queries, norm_prev, precision=lax.Precision.HIGHEST)
    from_memory = numer / denom[..., None]
    zero_seg = jnp.zeros((1, SEG, HEADS, HD), jnp.bfloat16)
    key_prev = jnp.concatenate([zero_seg, key_all[:-1]], axis=0)
    value_prev = jnp.concatenate([zero_seg, value_all[:-1]], axis=0)
    first_flags = (jnp.arange(segments) == 0).astype(jnp.int32)
    local = lax.map(segment_attention, (query_all, key_all, value_all, key_prev, value_prev, first_flags))
    gate = jax.nn.sigmoid(beta.astype(jnp.float32))[None, None, :, None]
    attended = (gate * from_memory + (1.0 - gate) * local).astype(jnp.bfloat16).reshape(TOKENS, HEADS * HD)
    return jnp.dot(attended, w_out, preferred_element_type=jnp.float32).astype(jnp.bfloat16)
```

```python
import functools

import jax
import jax.numpy as jnp
from jax import lax
from jax.experimental import pallas as pl
from jax.experimental.pallas import tpu as pltpu
from jax.sharding import PartitionSpec as P

HD = 128
SEG = 2048
CHUNKS = 2


def passed_along(block, axis, distance):
    devices = range(lax.axis_size(axis))
    route = [(i - distance, i) for i in devices if i - distance in devices]
    return lax.ppermute(block, axis, route)


def prefix(part, axis, combine, identity):
    place = lax.axis_index(axis)
    gathered = jax.tree.map(lambda a: lax.all_gather(a, axis), part)
    state = jax.tree.map(lambda a, e: jnp.zeros_like(a) + jnp.asarray(e, a.dtype), part, identity)

    def one(hop, state):
        return combine(
            state, jax.tree.map(lambda a: lax.dynamic_index_in_dim(a, hop, 0, False), gathered)
        )

    return lax.fori_loop(0, place, one, state)


def elu_plus(inputs):
    return jnp.where(inputs > 0, inputs + 1.0, jnp.exp(jnp.minimum(inputs, 0.0)))


def add_pair(earlier, later):
    return (earlier[0] + later[0], earlier[1] + later[1])


def memory_terms(key_block, value_block, heads_here, row_weight):
    token_rows = key_block.shape[0]
    soft_keys = elu_plus(key_block.astype(jnp.float32)).astype(jnp.bfloat16)
    soft_keys = (soft_keys * row_weight[:, None]).reshape(token_rows, heads_here, HD)
    shaped_values = value_block.reshape(token_rows, heads_here, HD)
    outer = jnp.einsum("thd,the->hde", soft_keys, shaped_values, preferred_element_type=jnp.float32)
    totals = jnp.sum(soft_keys, axis=0, dtype=jnp.float32)
    return (outer, totals)


def body(queries, keys, values, beta, w_out):
    token_rows, width = queries.shape
    heads_here = width // HD
    groups = SEG // token_rows
    seq_rank = lax.axis_index("seq")
    place = seq_rank % groups
    stacked = jnp.stack((keys, values))
    earlier_blocks = []
    moving = stacked
    for distance in range(1, groups + 1):
        moving = passed_along(moving, "seq", 1)
        earlier_blocks.append(moving)
    ordered = earlier_blocks[::-1] + [stacked]
    all_keys = jnp.concatenate([block[0] for block in ordered], axis=0)
    all_values = jnp.concatenate([block[1] for block in ordered], axis=0)
    own_ones = jnp.ones((token_rows,), jnp.bfloat16)
    own_outer, own_totals = memory_terms(keys, values, heads_here, own_ones)
    zero_mem = jnp.zeros((heads_here, HD, HD), jnp.float32)
    zero_norm = jnp.zeros((heads_here, HD), jnp.float32)
    memory, norm_prev = prefix((own_outer, own_totals), "seq", add_pair, (zero_mem, zero_norm))
    earlier_rows = groups * token_rows
    row_distance = groups - jnp.arange(earlier_rows) // token_rows
    inside = ((row_distance <= place) & (row_distance < groups)).astype(jnp.bfloat16)
    outer, totals = memory_terms(
        all_keys[:earlier_rows], all_values[:earlier_rows], heads_here, inside
    )
    memory = memory - outer
    norm_prev = norm_prev - totals
    soft_queries = lax.optimization_barrier(
        elu_plus(queries.astype(jnp.float32)).astype(jnp.bfloat16)
    )
    soft_queries = soft_queries.astype(jnp.float32).reshape(token_rows, heads_here, HD)
    numer = jnp.einsum("thd,hde->the", soft_queries, memory, precision=lax.Precision.HIGHEST)
    denom = 1.0 + jnp.einsum("thd,hd->th", soft_queries, norm_prev, precision=lax.Precision.HIGHEST)
    from_memory = numer / denom[..., None]
    scale = HD ** (-0.5)
    key_offset = jnp.arange((groups + 1) * token_rows) - groups * token_rows
    query_offset = jnp.arange(token_rows)
    visible = (
        (key_offset[None, :] <= query_offset[:, None])
        & (key_offset[None, :] > query_offset[:, None] - SEG)
        & (seq_rank * token_rows + key_offset[None, :] >= 0)
    )
    gates = jax.nn.sigmoid(beta)
    outputs = []
    for head_index in range(heads_here):
        lower = head_index * HD
        query_head = queries[:, lower : lower + HD]
        key_head = all_keys[:, lower : lower + HD]
        value_head = all_values[:, lower : lower + HD]
        scores = (
            lax.dot_general(
                query_head, key_head, (((1,), (1,)), ((), ())), preferred_element_type=jnp.float32
            )
            * scale
        )
        scores = jnp.where(visible, scores, -jnp.inf)
        highest = jnp.max(scores, axis=1, keepdims=True)
        weights = jnp.exp(scores - highest)
        total = jnp.sum(weights, axis=1, keepdims=True)
        local = (
            jnp.dot(weights.astype(jnp.bfloat16), value_head, preferred_element_type=jnp.float32)
            / total
        )
        gate = gates[head_index]
        outputs.append(
            (gate * from_memory[:, head_index] + (1.0 - gate) * local).astype(jnp.bfloat16)
        )
    attended = jnp.concatenate(outputs, axis=1)
    partial_out = jnp.dot(attended, w_out, preferred_element_type=jnp.float32)
    summed = lax.psum_scatter(partial_out, "head", scatter_dimension=1, tiled=True)
    return summed.astype(jnp.bfloat16)


def exchange_kernel(
    n_seq, n_head, heads, chunks, beta_ref, q_hbm, k_hbm, v_hbm, w_hbm, out_ref,
    k_all, v_all, q_all, o_all, q_own, gated_memory, memory, norm_prev, local_own, w_own,
    to_sibling, from_sibling, kept, to_far, from_far,
    in_send, in_recv, own_sem, o_send, o_recv, sib_send, sib_recv, far_send, far_recv,
):
    me = lax.axis_index("seq")
    head_rank = lax.axis_index("head")
    pair = head_rank // 2
    side = head_rank % 2
    pairs = n_head // 2
    sibling = pair * 2 + 1 - side
    rows = q_own.shape[0]
    part = rows // chunks
    out_cols = out_ref.shape[1]
    offsets = sorted(range(1, n_seq), key=lambda d: abs(d - n_seq // 2))

    def remote(src, dst, send, recv, where):
        return pltpu.make_async_remote_copy(
            src_ref=src, dst_ref=dst, send_sem=send, recv_sem=recv,
            device_id=where, device_id_type=pl.DeviceIdType.MESH,
        )

    barrier = pltpu.get_barrier_semaphore()
    for d in range(1, n_seq):
        pl.semaphore_signal(
            barrier, inc=1, device_id={"seq": (me + d) % n_seq},
            device_id_type=pl.DeviceIdType.MESH,
        )
    pl.semaphore_signal(
        barrier, inc=1, device_id={"head": sibling}, device_id_type=pl.DeviceIdType.MESH
    )
    for hop in range(1, pairs):
        pl.semaphore_signal(
            barrier, inc=1, device_id={"head": ((pair + hop) % pairs) * 2 + side},
            device_id_type=pl.DeviceIdType.MESH,
        )
    pl.semaphore_wait(barrier, n_seq - 1 + 1 + pairs - 1)

    def lanes(index):
        return pl.ds(pl.multiple_of(index * HD, HD), HD)

    def place(index, start, size):
        return pl.ds(pl.multiple_of(index * rows + start, part), size)

    def inbound(kind, d):
        target = (me + d) % n_seq
        if kind < 2:
            src, dst, start, size = (k_hbm, k_all, 0, rows) if kind == 0 else (v_hbm, v_all, 0, rows)
        else:
            src, dst, start, size = q_hbm, q_all, (kind - 2) * part, part
        return remote(
            src.at[pl.ds(start, size), lanes(target)], dst.at[place(me, start, size), :],
            in_send.at[kind, d], in_recv.at[kind, d], {"seq": target},
        )

    for kind_group in [(0, 1)] + [(2 + c,) for c in range(chunks)]:
        for d in offsets:
            for kind in kind_group:
                inbound(kind, d).start()

    own_copies = [
        pltpu.make_async_copy(k_hbm.at[:, lanes(me)], k_all.at[place(me, 0, rows), :], own_sem.at[0]),
        pltpu.make_async_copy(v_hbm.at[:, lanes(me)], v_all.at[place(me, 0, rows), :], own_sem.at[1]),
        pltpu.make_async_copy(q_hbm.at[:, lanes(me)], q_all.at[place(me, 0, rows), :], own_sem.at[2]),
        pltpu.make_async_copy(q_hbm, q_own, own_sem.at[3]),
        pltpu.make_async_copy(w_hbm, w_own, own_sem.at[4]),
    ]
    for copy in own_copies:
        copy.start()

    memory[...] = jnp.zeros_like(memory)
    norm_prev[...] = jnp.zeros_like(norm_prev)
    own_copies[3].wait()
    for h in range(heads):
        cols = slice(h * HD, (h + 1) * HD)
        soft = elu_plus(q_own[:, cols].astype(jnp.float32)).astype(jnp.bfloat16).astype(jnp.float32)
        numer = jnp.dot(
            soft, memory[h], precision=lax.Precision.HIGHEST, preferred_element_type=jnp.float32
        )
        denom = 1.0 + jnp.sum(soft * norm_prev[h : h + 1, :], axis=1, keepdims=True)
        gate = jax.nn.sigmoid(jnp.full((1, HD), beta_ref[h], jnp.float32))
        gated_memory[:, cols] = gate * (numer / denom)
    for index in range(3):
        own_copies[index].wait()

    def arrived(kind, source):
        d = (me - source + n_seq) % n_seq

        @pl.when(source != me)
        def _():
            start, size = (0, rows) if kind < 2 else ((kind - 2) * part, part)
            dst = (k_all, v_all, q_all)[min(kind, 2)].at[place(source, start, size), :]
            remote(dst, dst, in_send.at[kind, d], in_recv.at[kind, d], {"seq": source}).wait_recv()

    keep_local = 1.0 - jax.nn.sigmoid(jnp.full((1, HD), beta_ref[me], jnp.float32))
    factor = HD ** (-0.5) * 1.4426950408889634
    row_at = lax.broadcasted_iota(jnp.int32, (part, part), 0)
    col_at = lax.broadcasted_iota(jnp.int32, (part, part), 1)
    contract = (((1,), (1,)), ((), ()))

    def outbound(chunk, block):
        d = (block - me + n_seq) % n_seq
        return remote(
            o_all.at[pl.ds(block * rows + chunk * part, part), :],
            local_own.at[pl.ds(chunk * part, part), lanes(me)],
            o_send.at[chunk, d], o_recv.at[chunk, d], {"seq": block},
        )

    for chunk in range(chunks):
        for block in range(n_seq):
            if chunk == 0:
                arrived(0, block)
                arrived(1, block)
            arrived(2 + chunk, block)
            first = block * rows + chunk * part
            query = q_all[first : first + part, :]
            edge = lax.dot_general(
                query, k_all[first : first + part, :], contract, preferred_element_type=jnp.float32
            )
            edge = jnp.where(col_at <= row_at, edge, -jnp.inf)
            highest = jnp.max(edge, axis=1, keepdims=True)
            if first:
                scores = lax.dot_general(
                    query, k_all[:first, :], contract, preferred_element_type=jnp.float32
                )
                highest = jnp.maximum(highest, jnp.max(scores, axis=1, keepdims=True))
            weights = jnp.exp2((edge - highest) * factor)
            total = jnp.sum(weights, axis=1, keepdims=True)
            summed = jnp.dot(
                weights.astype(jnp.bfloat16), v_all[first : first + part, :],
                preferred_element_type=jnp.float32,
            )
            if first:
                weights = jnp.exp2((scores - highest) * factor)
                total = total + jnp.sum(weights, axis=1, keepdims=True)
                summed = summed + jnp.dot(
                    weights.astype(jnp.bfloat16), v_all[:first, :],
                    preferred_element_type=jnp.float32,
                )
            result = (keep_local * (summed / total)).astype(jnp.bfloat16)
            o_all[first : first + part, :] = result

            @pl.when(block != me)
            def _():
                outbound(chunk, block).start()

            @pl.when(block == me)
            def _():
                local_own[chunk * part : (chunk + 1) * part, lanes(me)] = result

    own_copies[4].wait()

    def sibling_copy(chunk, hop):
        return remote(
            to_sibling.at[chunk, hop], from_sibling.at[chunk, hop],
            sib_send.at[chunk, hop], sib_recv.at[chunk, hop], {"head": sibling},
        )

    def far_copy(chunk, hop):
        return remote(
            to_far.at[chunk, hop - 1], from_far.at[chunk, hop - 1],
            far_send.at[chunk, hop - 1], far_recv.at[chunk, hop - 1],
            {"head": ((pair + hop) % pairs) * 2 + side},
        )

    hops = list(range(1, pairs)) + [0]
    for chunk in range(chunks):
        span = slice(chunk * part, (chunk + 1) * part)
        for d in range(1, n_seq):
            source = (me - d + n_seq) % n_seq
            dst = local_own.at[pl.ds(chunk * part, part), lanes(source)]
            remote(dst, dst, o_send.at[chunk, d], o_recv.at[chunk, d], {"seq": source}).wait_recv()
        attended = (local_own[span, :].astype(jnp.float32) + gated_memory[span, :]).astype(jnp.bfloat16)

        def share(index):
            cols = pl.ds(pl.multiple_of(index * out_cols, out_cols), out_cols)
            return jnp.dot(attended, w_own[:, cols], preferred_element_type=jnp.float32)

        for hop in hops:
            base = ((pair + hop) % pairs) * 2
            to_sibling[chunk, hop] = share(base + 1 - side).astype(jnp.bfloat16)
            sibling_copy(chunk, hop).start()
            kept[chunk, hop] = share(base + side)
            if hop:
                sibling_copy(chunk, hop).wait_recv()
                to_far[chunk, hop - 1] = (
                    kept[chunk, hop] + from_sibling[chunk, hop].astype(jnp.float32)
                ).astype(jnp.bfloat16)
                far_copy(chunk, hop).start()

    for chunk in range(chunks):
        span = slice(chunk * part, (chunk + 1) * part)
        sibling_copy(chunk, 0).wait_recv()
        result = kept[chunk, 0] + from_sibling[chunk, 0].astype(jnp.float32)
        for hop in range(1, pairs):
            far_copy(chunk, hop).wait_recv()
            result = result + from_far[chunk, hop - 1].astype(jnp.float32)
        out_ref[span, :] = result.astype(out_ref.dtype)

    for kind in range(2 + chunks):
        for d in offsets:
            inbound(kind, d).wait_send()
    for chunk in range(chunks):
        for block in range(n_seq):
            @pl.when(block != me)
            def _():
                outbound(chunk, block).wait_send()
        for hop in range(pairs):
            sibling_copy(chunk, hop).wait_send()
            if hop:
                far_copy(chunk, hop).wait_send()


def one_segment_body(n_seq, n_head, queries, keys, values, beta, w_out):
    rows, width = queries.shape
    heads = width // HD
    tokens = rows * n_seq
    out_cols = w_out.shape[1] // n_head
    pairs = n_head // 2
    chunks = CHUNKS
    part = rows // chunks
    vmem, dma = pltpu.VMEM, pltpu.SemaphoreType.DMA
    half, full = jnp.bfloat16, jnp.float32
    anywhere = pl.BlockSpec(memory_space=pl.ANY)
    return pl.pallas_call(
        functools.partial(exchange_kernel, n_seq, n_head, heads, chunks),
        out_shape=jax.ShapeDtypeStruct((rows, out_cols), half),
        in_specs=[pl.BlockSpec(memory_space=pltpu.SMEM)] + [anywhere] * 4,
        out_specs=pl.BlockSpec(memory_space=pltpu.VMEM),
        scratch_shapes=[
            vmem((tokens, HD), half), vmem((tokens, HD), half), vmem((tokens, HD), half),
            vmem((tokens, HD), half), vmem((rows, width), half), vmem((rows, width), full),
            vmem((heads, HD, HD), full), vmem((heads, HD), full), vmem((rows, width), half),
            vmem(w_out.shape, half),
            vmem((chunks, pairs, part, out_cols), half), vmem((chunks, pairs, part, out_cols), half),
            vmem((chunks, pairs, part, out_cols), full),
            vmem((chunks, max(pairs - 1, 1), part, out_cols), half),
            vmem((chunks, max(pairs - 1, 1), part, out_cols), half),
            dma((2 + chunks, n_seq)), dma((2 + chunks, n_seq)), dma((5,)),
            dma((chunks, n_seq)), dma((chunks, n_seq)),
            dma((chunks, pairs)), dma((chunks, pairs)),
            dma((chunks, max(pairs - 1, 1))), dma((chunks, max(pairs - 1, 1))),
        ],
        compiler_params=pltpu.CompilerParams(
            collective_id=0, has_side_effects=True, vmem_limit_bytes=50 * 1024 * 1024
        ),
    )(beta, queries, keys, values, w_out)


def solution(mesh):
    placed = (P("seq", "head"), P("seq", "head"), P("seq", "head"), P("head"), P("head", None))
    n_seq, n_head = mesh.shape["seq"], mesh.shape["head"]

    def chosen(queries, keys, values, beta, w_out):
        rows, width = queries.shape
        if rows * n_seq == SEG and width == HD * n_seq and n_head % 2 == 0:
            return one_segment_body(n_seq, n_head, queries, keys, values, beta, w_out)
        return body(queries, keys, values, beta, w_out)

    return jax.shard_map(
        chosen, mesh=mesh, in_specs=placed, out_specs=P("seq", "head"), check_vma=False
    )
```

```python
import functools

import jax
import jax.numpy as jnp
from jax import lax
from jax.experimental import pallas as pl
from jax.experimental.pallas import tpu as pltpu
from jax.sharding import PartitionSpec as P

HD = 128
SEG = 2048
CHUNKS = 2
QUARTERS = 4


def passed_along(block, axis, distance):
    devices = range(lax.axis_size(axis))
    route = [(i - distance, i) for i in devices if i - distance in devices]
    return lax.ppermute(block, axis, route)


def prefix(part, axis, combine, identity):
    place = lax.axis_index(axis)
    gathered = jax.tree.map(lambda a: lax.all_gather(a, axis), part)
    state = jax.tree.map(lambda a, e: jnp.zeros_like(a) + jnp.asarray(e, a.dtype), part, identity)

    def one(hop, state):
        return combine(
            state, jax.tree.map(lambda a: lax.dynamic_index_in_dim(a, hop, 0, False), gathered)
        )

    return lax.fori_loop(0, place, one, state)


def elu_plus(inputs):
    return jnp.where(inputs > 0, inputs + 1.0, jnp.exp(jnp.minimum(inputs, 0.0)))


def add_pair(earlier, later):
    return (earlier[0] + later[0], earlier[1] + later[1])


def memory_terms(key_block, value_block, heads_here, row_weight):
    token_rows = key_block.shape[0]
    soft_keys = elu_plus(key_block.astype(jnp.float32)).astype(jnp.bfloat16)
    soft_keys = (soft_keys * row_weight[:, None]).reshape(token_rows, heads_here, HD)
    shaped_values = value_block.reshape(token_rows, heads_here, HD)
    outer = jnp.einsum("thd,the->hde", soft_keys, shaped_values, preferred_element_type=jnp.float32)
    totals = jnp.sum(soft_keys, axis=0, dtype=jnp.float32)
    return (outer, totals)


def body(queries, keys, values, beta, w_out):
    token_rows, width = queries.shape
    heads_here = width // HD
    groups = SEG // token_rows
    seq_rank = lax.axis_index("seq")
    place = seq_rank % groups
    stacked = jnp.stack((keys, values))
    earlier_blocks = []
    moving = stacked
    for distance in range(1, groups + 1):
        moving = passed_along(moving, "seq", 1)
        earlier_blocks.append(moving)
    ordered = earlier_blocks[::-1] + [stacked]
    all_keys = jnp.concatenate([block[0] for block in ordered], axis=0)
    all_values = jnp.concatenate([block[1] for block in ordered], axis=0)
    own_ones = jnp.ones((token_rows,), jnp.bfloat16)
    own_outer, own_totals = memory_terms(keys, values, heads_here, own_ones)
    zero_mem = jnp.zeros((heads_here, HD, HD), jnp.float32)
    zero_norm = jnp.zeros((heads_here, HD), jnp.float32)
    memory, norm_prev = prefix((own_outer, own_totals), "seq", add_pair, (zero_mem, zero_norm))
    earlier_rows = groups * token_rows
    row_distance = groups - jnp.arange(earlier_rows) // token_rows
    inside = ((row_distance <= place) & (row_distance < groups)).astype(jnp.bfloat16)
    outer, totals = memory_terms(
        all_keys[:earlier_rows], all_values[:earlier_rows], heads_here, inside
    )
    memory = memory - outer
    norm_prev = norm_prev - totals
    soft_queries = lax.optimization_barrier(
        elu_plus(queries.astype(jnp.float32)).astype(jnp.bfloat16)
    )
    soft_queries = soft_queries.astype(jnp.float32).reshape(token_rows, heads_here, HD)
    numer = jnp.einsum("thd,hde->the", soft_queries, memory, precision=lax.Precision.HIGHEST)
    denom = 1.0 + jnp.einsum("thd,hd->th", soft_queries, norm_prev, precision=lax.Precision.HIGHEST)
    from_memory = numer / denom[..., None]
    scale = HD ** (-0.5)
    key_offset = jnp.arange((groups + 1) * token_rows) - groups * token_rows
    query_offset = jnp.arange(token_rows)
    visible = (
        (key_offset[None, :] <= query_offset[:, None])
        & (key_offset[None, :] > query_offset[:, None] - SEG)
        & (seq_rank * token_rows + key_offset[None, :] >= 0)
    )
    gates = jax.nn.sigmoid(beta)
    outputs = []
    for head_index in range(heads_here):
        lower = head_index * HD
        query_head = queries[:, lower : lower + HD]
        key_head = all_keys[:, lower : lower + HD]
        value_head = all_values[:, lower : lower + HD]
        scores = (
            lax.dot_general(
                query_head, key_head, (((1,), (1,)), ((), ())), preferred_element_type=jnp.float32
            )
            * scale
        )
        scores = jnp.where(visible, scores, -jnp.inf)
        highest = jnp.max(scores, axis=1, keepdims=True)
        weights = jnp.exp(scores - highest)
        total = jnp.sum(weights, axis=1, keepdims=True)
        local = (
            jnp.dot(weights.astype(jnp.bfloat16), value_head, preferred_element_type=jnp.float32)
            / total
        )
        gate = gates[head_index]
        outputs.append(
            (gate * from_memory[:, head_index] + (1.0 - gate) * local).astype(jnp.bfloat16)
        )
    attended = jnp.concatenate(outputs, axis=1)
    partial_out = jnp.dot(attended, w_out, preferred_element_type=jnp.float32)
    summed = lax.psum_scatter(partial_out, "head", scatter_dimension=1, tiled=True)
    return summed.astype(jnp.bfloat16)


def exchange_kernel(
    n_seq, n_head, heads, chunks, beta_ref, q_hbm, k_hbm, v_hbm, w_hbm, out_ref,
    k_all, v_all, q_all, o_all, sums_all, q_own, gated_memory, memory, norm_prev,
    parts, sums, attended_own, w_own,
    to_sibling, from_sibling, kept, to_far, from_far,
    in_send, in_recv, own_sem, o_send, o_recv, sums_send, sums_recv,
    sib_send, sib_recv, far_send, far_recv,
):
    me = lax.axis_index("seq")
    head_rank = lax.axis_index("head")
    pair = head_rank // 2
    side = head_rank % 2
    pairs = n_head // 2
    sibling = pair * 2 + 1 - side
    rows = q_own.shape[0]
    part = rows // chunks
    out_cols = out_ref.shape[1]
    group = n_seq // QUARTERS
    quarter = me // group
    mine = me % group
    many = heads // group
    wide = many * HD
    held = group * rows

    def remote(src, dst, send, recv, where):
        return pltpu.make_async_remote_copy(
            src_ref=src, dst_ref=dst, send_sem=send, recv_sem=recv,
            device_id=where, device_id_type=pl.DeviceIdType.MESH,
        )

    barrier = pltpu.get_barrier_semaphore()
    for d in range(1, n_seq):
        pl.semaphore_signal(
            barrier, inc=1, device_id={"seq": (me + d) % n_seq},
            device_id_type=pl.DeviceIdType.MESH,
        )
    pl.semaphore_signal(
        barrier, inc=1, device_id={"head": sibling}, device_id_type=pl.DeviceIdType.MESH
    )
    for hop in range(1, pairs):
        pl.semaphore_signal(
            barrier, inc=1, device_id={"head": ((pair + hop) % pairs) * 2 + side},
            device_id_type=pl.DeviceIdType.MESH,
        )
    pl.semaphore_wait(barrier, n_seq - 1 + 1 + pairs - 1)

    def lanes(index):
        return pl.ds(pl.multiple_of(index * HD, HD), HD)

    sources = (k_hbm, v_hbm, q_hbm, k_hbm, v_hbm, q_hbm, q_hbm)
    landing = (k_all, v_all, q_all, k_all, v_all, q_all, q_all)
    base_row = (held, held, 0, 0, 0, held, 2 * held)

    def moved(kind, channel, head, there, to_quarter):
        return remote(
            sources[kind].at[:, lanes(there * many + head)],
            landing[kind].at[
                pl.ds(pl.multiple_of(base_row[kind] + mine * rows, rows), rows), lanes(head)
            ],
            in_send.at[channel, head, there], in_recv.at[kind, head, mine],
            {"seq": to_quarter * group + there},
        )

    def landed(kind, head, source):
        dst = landing[kind].at[pl.ds(base_row[kind] + source * rows, rows), lanes(head)]
        return remote(
            dst, dst, in_send.at[kind, head, source], in_recv.at[kind, head, source],
            {"seq": (me + 1) % n_seq},
        )

    def plan(role):
        sends = []
        if role == 0:
            sends += [(3, 3, 1), (4, 4, 1)]
        if role == 2:
            sends += [(5, 5, 1)]
        if role == 3:
            sends += [(6, 5, 1), (6, 6, 2)]
        return sends

    def in_role(role, action):
        pl.when(quarter == role)(action)

    def each_send(role, action):
        def one(head, carry):
            for kind, channel, to_quarter in plan(role):
                for there in range(group):
                    action(moved(kind, channel, head, there, to_quarter))
            for there in range(group):
                @pl.when(there != mine)
                def _():
                    for kind in range(3):
                        action(moved(kind, kind, head, there, role))
            return carry

        lax.fori_loop(0, many, one, 0)

    for role in range(QUARTERS):
        in_role(role, functools.partial(each_send, role, lambda copy: copy.start()))

    block = pl.ds(pl.multiple_of(mine * wide, wide), wide)
    own_copies = [
        pltpu.make_async_copy(
            source.at[:, block],
            place.at[pl.ds(pl.multiple_of(start + mine * rows, rows), rows), :], own_sem.at[i],
        )
        for i, (source, place, start) in enumerate(
            ((k_hbm, k_all, held), (v_hbm, v_all, held), (q_hbm, q_all, 0))
        )
    ]
    own_copies += [
        pltpu.make_async_copy(q_hbm, q_own, own_sem.at[3]),
        pltpu.make_async_copy(w_hbm, w_own, own_sem.at[4]),
    ]
    for copy in own_copies:
        copy.start()

    memory[...] = jnp.zeros_like(memory)
    norm_prev[...] = jnp.zeros_like(norm_prev)
    own_copies[3].wait()

    def gate_of(h):
        return jax.nn.sigmoid(jnp.full((1, HD), beta_ref[h], jnp.float32))

    for h in range(heads):
        cols = slice(h * HD, (h + 1) * HD)
        soft = elu_plus(q_own[:, cols].astype(jnp.float32)).astype(jnp.bfloat16).astype(jnp.float32)
        numer = jnp.dot(
            soft, memory[h], precision=lax.Precision.HIGHEST, preferred_element_type=jnp.float32
        )
        denom = 1.0 + jnp.sum(soft * norm_prev[h : h + 1, :], axis=1, keepdims=True)
        gated_memory[:, cols] = gate_of(h) * (numer / denom)

    for slot in (1, 2):
        @pl.when(quarter <= slot)
        def _():
            parts[slot] = jnp.zeros(parts.shape[1:], parts.dtype)
            sums[slot] = jnp.full(sums.shape[1:], -1e30, sums.dtype)

    for index in range(3):
        own_copies[index].wait()

    factor = HD ** (-0.5) * 1.4426950408889634
    contract = (((1,), (1,)), ((), ()))

    def tile(query, cols, low, high, edge_size):
        pieces = []
        split = high - edge_size
        if edge_size:
            size = query.shape[0]
            edge = lax.dot_general(
                query, k_all[split:high, cols], contract, preferred_element_type=jnp.float32
            )
            row_at = lax.broadcasted_iota(jnp.int32, (size, edge_size), 0)
            col_at = lax.broadcasted_iota(jnp.int32, (size, edge_size), 1)
            pieces.append((jnp.where(col_at <= row_at, edge, -jnp.inf), split, high))
        if split > low:
            scores = lax.dot_general(
                query, k_all[low:split, cols], contract, preferred_element_type=jnp.float32
            )
            pieces.append((scores, low, split))
        highest = functools.reduce(
            jnp.maximum, [jnp.max(p, axis=1, keepdims=True) for p, _, _ in pieces]
        )
        total, summed = 0.0, 0.0
        for scores, first, last in pieces:
            weights = jnp.exp2((scores - highest) * factor)
            total = total + jnp.sum(weights, axis=1, keepdims=True)
            summed = summed + jnp.dot(
                weights.astype(jnp.bfloat16), v_all[first:last, cols],
                preferred_element_type=jnp.float32,
            )
        level = highest * factor + jnp.log(total) * 1.4426950408889634
        return (summed / total).astype(jnp.bfloat16), level

    def returned(q_slot, head, there, to_quarter, slot):
        where = {"seq": to_quarter * group + there}
        index = mine * many + head
        return (
            remote(
                o_all.at[q_slot, there, :, lanes(head)], parts.at[slot, :, lanes(index)],
                o_send.at[q_slot, head, there], o_recv.at[slot, index], where,
            ),
            remote(
                sums_all.at[q_slot, there, head], sums.at[slot, index],
                sums_send.at[q_slot, head, there], sums_recv.at[slot, index], where,
            ),
        )

    def run_block(q_slot, head, there, low, causal):
        cols = lanes(head)
        for start in range(0, rows, part):
            at = there * rows + start
            query = q_all[q_slot * held + at : q_slot * held + at + part, cols]
            high = held + at + part if causal else 2 * held
            out, level = tile(query, cols, low, high, part if causal else 0)
            o_all[q_slot, there, start : start + part, cols] = out
            turned = jnp.transpose(jnp.broadcast_to(level, (part, HD)))
            sums_all[q_slot, there, head, :, start : start + part] = turned[:1, :]

    def wait_pair(head, kinds, own):
        for source in range(group):
            def go():
                for kind in kinds:
                    landed(kind, head, source).wait_recv()
            if own:
                pl.when(source != mine)(go)
            else:
                go()

    away = {1: [(1, 5, 0, 2, 1), (2, 6, 0, 3, 1)], 2: [(2, 6, held, 3, 2)]}

    def attend(role):
        low = 0 if role == 1 else held

        def one(head, carry):
            wait_pair(head, (0, 1, 2), True)
            if role == 1:
                wait_pair(head, (3, 4), False)
            for q_slot, kind, first, to_quarter, slot in away.get(role, []):
                for there in range(group):
                    landed(kind, head, there).wait_recv()
                    run_block(q_slot, head, there, first, False)
                    for copy in returned(q_slot, head, there, to_quarter, slot):
                        copy.start()
            for there in range(group):
                run_block(0, head, there, low, True)

                @pl.when(there != mine)
                def _():
                    for copy in returned(0, head, there, role, 0):
                        copy.start()

                @pl.when(there == mine)
                def _():
                    index = mine * many + head
                    parts[0, :, lanes(index)] = o_all[0, there, :, lanes(head)]
                    sums[0, index] = sums_all[0, there, head]
            return carry

        lax.fori_loop(0, many, one, 0)

    for role in range(QUARTERS):
        in_role(role, functools.partial(attend, role))

    def wait_part(slot, index):
        dst, level = parts.at[slot, :, lanes(index)], sums.at[slot, index]
        where = {"seq": (me + 1) % n_seq}
        remote(dst, dst, o_send.at[0, 0, 0], o_recv.at[slot, index], where).wait_recv()
        remote(level, level, sums_send.at[0, 0, 0], sums_recv.at[slot, index], where).wait_recv()

    def merge(head, carry):
        for there in range(group):
            index = there * many + head

            @pl.when(there != mine)
            def _():
                wait_part(0, index)

            for slot in (1, 2):
                @pl.when(quarter > slot)
                def _():
                    wait_part(slot, index)

            for start in range(0, rows, part):
                span = slice(start, start + part)
                levels = [
                    jnp.transpose(jnp.broadcast_to(sums[slot, index, :, span], (HD, part)))
                    for slot in range(3)
                ]
                top = functools.reduce(jnp.maximum, levels)
                shares = [jnp.exp2(level - top) for level in levels]
                mixed = sum(
                    share * parts[slot, span, lanes(index)].astype(jnp.float32)
                    for slot, share in enumerate(shares)
                )
                local = mixed / sum(shares)
                attended_own[span, lanes(index)] = (
                    gated_memory[span, lanes(index)] + (1.0 - gate_of(index)) * local
                ).astype(jnp.bfloat16)
        return carry

    lax.fori_loop(0, many, merge, 0)

    own_copies[4].wait()

    def sibling_copy(chunk, hop):
        return remote(
            to_sibling.at[chunk, hop], from_sibling.at[chunk, hop],
            sib_send.at[chunk, hop], sib_recv.at[chunk, hop], {"head": sibling},
        )

    def far_copy(chunk, hop):
        return remote(
            to_far.at[chunk, hop - 1], from_far.at[chunk, hop - 1],
            far_send.at[chunk, hop - 1], far_recv.at[chunk, hop - 1],
            {"head": ((pair + hop) % pairs) * 2 + side},
        )

    hops = list(range(1, pairs)) + [0]
    for chunk in range(chunks):
        span = slice(chunk * part, (chunk + 1) * part)
        attended = attended_own[span, :]

        def share(index):
            cols = pl.ds(pl.multiple_of(index * out_cols, out_cols), out_cols)
            return jnp.dot(attended, w_own[:, cols], preferred_element_type=jnp.float32)

        for hop in hops:
            base = ((pair + hop) % pairs) * 2
            to_sibling[chunk, hop] = share(base + 1 - side).astype(jnp.bfloat16)
            sibling_copy(chunk, hop).start()
            kept[chunk, hop] = share(base + side)
            if hop:
                sibling_copy(chunk, hop).wait_recv()
                to_far[chunk, hop - 1] = (
                    kept[chunk, hop] + from_sibling[chunk, hop].astype(jnp.float32)
                ).astype(jnp.bfloat16)
                far_copy(chunk, hop).start()

    for chunk in range(chunks):
        span = slice(chunk * part, (chunk + 1) * part)
        sibling_copy(chunk, 0).wait_recv()
        result = kept[chunk, 0] + from_sibling[chunk, 0].astype(jnp.float32)
        for hop in range(1, pairs):
            far_copy(chunk, hop).wait_recv()
            result = result + from_far[chunk, hop - 1].astype(jnp.float32)
        out_ref[span, :] = result.astype(out_ref.dtype)

    for role in range(QUARTERS):
        def finish(role=role):
            each_send(role, lambda copy: copy.wait_send())

            def one(head, carry):
                for q_slot, _, _, to_quarter, slot in away.get(role, []):
                    for there in range(group):
                        for copy in returned(q_slot, head, there, to_quarter, slot):
                            copy.wait_send()
                for there in range(group):
                    @pl.when(there != mine)
                    def _():
                        for copy in returned(0, head, there, role, 0):
                            copy.wait_send()
                return carry

            lax.fori_loop(0, many, one, 0)

        in_role(role, finish)
    for chunk in range(chunks):
        for hop in range(pairs):
            sibling_copy(chunk, hop).wait_send()
            if hop:
                far_copy(chunk, hop).wait_send()


def one_segment_body(n_seq, n_head, queries, keys, values, beta, w_out):
    rows, width = queries.shape
    heads = width // HD
    group = n_seq // QUARTERS
    many = heads // group
    wide, held = many * HD, group * rows
    out_cols = w_out.shape[1] // n_head
    pairs = n_head // 2
    chunks = CHUNKS
    part = rows // chunks
    vmem, dma = pltpu.VMEM, pltpu.SemaphoreType.DMA
    half, full = jnp.bfloat16, jnp.float32
    anywhere = pl.BlockSpec(memory_space=pl.ANY)
    return pl.pallas_call(
        functools.partial(exchange_kernel, n_seq, n_head, heads, chunks),
        out_shape=jax.ShapeDtypeStruct((rows, out_cols), half),
        in_specs=[pl.BlockSpec(memory_space=pltpu.SMEM)] + [anywhere] * 4,
        out_specs=pl.BlockSpec(memory_space=pltpu.VMEM),
        scratch_shapes=[
            vmem((2 * held, wide), half), vmem((2 * held, wide), half), vmem((3 * held, wide), half),
            vmem((3, group, rows, wide), half), vmem((3, group, many, 1, rows), full),
            vmem((rows, width), half), vmem((rows, width), full),
            vmem((heads, HD, HD), full), vmem((heads, HD), full),
            vmem((3, rows, width), half), vmem((3, heads, 1, rows), full),
            vmem((rows, width), half), vmem(w_out.shape, half),
            vmem((chunks, pairs, part, out_cols), half), vmem((chunks, pairs, part, out_cols), half),
            vmem((chunks, pairs, part, out_cols), full),
            vmem((chunks, max(pairs - 1, 1), part, out_cols), half),
            vmem((chunks, max(pairs - 1, 1), part, out_cols), half),
            dma((7, many, group)), dma((7, many, group)), dma((5,)),
            dma((3, many, group)), dma((3, heads)), dma((3, many, group)), dma((3, heads)),
            dma((chunks, pairs)), dma((chunks, pairs)),
            dma((chunks, max(pairs - 1, 1))), dma((chunks, max(pairs - 1, 1))),
        ],
        compiler_params=pltpu.CompilerParams(
            collective_id=0, has_side_effects=True, vmem_limit_bytes=50 * 1024 * 1024
        ),
    )(beta, queries, keys, values, w_out)


def solution(mesh):
    placed = (P("seq", "head"), P("seq", "head"), P("seq", "head"), P("head"), P("head", None))
    n_seq, n_head = mesh.shape["seq"], mesh.shape["head"]

    def chosen(queries, keys, values, beta, w_out):
        rows, width = queries.shape
        fits = rows == CHUNKS * HD and n_head % 2 == 0 and width // HD * QUARTERS % n_seq == 0
        if rows * n_seq == SEG and n_seq % QUARTERS == 0 and fits:
            return one_segment_body(n_seq, n_head, queries, keys, values, beta, w_out)
        return body(queries, keys, values, beta, w_out)

    return jax.shard_map(
        chosen, mesh=mesh, in_specs=placed, out_specs=P("seq", "head"), check_vma=False
    )
```
